1024 devices in a mesh: node: 32 (over z, core), local: 32 (over y, x).
Axes of the slice: x: 4, y: 8, z: 16, core: 2. Of those that a mesh axis runs over, the one named last changes fastest.
Arguments:
- tokens: bfloat16 [8192, 3584], P(('node', 'local')), may hold values from -6 to 6
- expert_ids: int32 [8192, 4], P(('node', 'local')), may hold values from 0 to 127, as said below
- combine_codes: int32 [8192, 4], P(('node', 'local')), may hold values from 1 to 16
- gate_weight: bfloat16 [1024, 3584, 128], P(('node', 'local')), may hold values from -0.09375 to 0.09375
- up_weight: bfloat16 [1024, 3584, 128], P(('node', 'local')), may hold values from -0.09375 to 0.09375
- down_weight: bfloat16 [1024, 128, 3584], P(('node', 'local')), may hold values from -0.1875 to 0.1875
Outputs:
- moe_out: bfloat16 [8192, 3584], P(('node', 'local'))
The draws below stay inside these ranges and needn't reach their ends.
Inputs may be any that keep to these rules, and one draw needn't show every extreme that they name: `expert_ids`: expert e belongs to node group e // 4. A token never names two experts of one node group. The 4 ids of each block of 8 rows (the rows of one device) name every node group exactly 1 times. Over all rows r with one value of (r // 8) % 32, no expert is named more than 16 times, and in every node group some expert is named exactly that often.
All inputs are finite; a program needn't handle non-finite values.
Results may differ from the reference program's by a relative error of at most 0.011.
Values may be sent and summed in bfloat16 or wider, within the bound.
No kernel may reach another device: no remote copies, remote signals or barrier semaphores. Data moves between devices by JAX's collectives and lax.ppermute only.
A program may use at most 32 MiB of HBM per device.

```python
import jax
import jax.numpy as jnp
from jax import lax

D = 3584
FF = 1024
TOP = 4
EXP_NODE = 4
TOK_DEV = 8
SLICES = 8
H_DEV = 128
EXPERTS = 128
NODE_ROUTES = 1
EXPERT_CAP = 16
TOKENS = 8192
N_NODE = 32
N_LOCAL = 32


def draw_expert_ids(key, part):
    base_key = jax.random.fold_in(key, 11)
    key_nodes, key_hot, key_order = jax.random.split(base_key, 3)
    devices_all = N_NODE * N_LOCAL
    routes_dev = TOK_DEV * TOP
    node_perms = jax.vmap(lambda subkey: jax.random.permutation(subkey, N_NODE))(jax.random.split(key_nodes, devices_all)).astype(jnp.int32)
    route_index = jnp.arange(routes_dev, dtype=jnp.int32)
    target_node = node_perms[:, route_index % N_NODE]
    device_index = jnp.arange(devices_all, dtype=jnp.int32)
    source_node = device_index // N_LOCAL
    source_local = device_index % N_LOCAL
    position = source_node[:, None] * NODE_ROUTES + (route_index // N_NODE)[None, :]
    hottest = jax.random.randint(key_hot, (N_NODE, N_LOCAL), 0, EXP_NODE).astype(jnp.int32)
    others = max(EXP_NODE - 1, 1)
    offset = jnp.where(route_index < EXPERT_CAP, 0, 1 + (route_index - EXPERT_CAP) % others).astype(jnp.int32)
    member_slot = (hottest[:, :, None] + offset[None, None, :]) % EXP_NODE
    shuffles = jax.vmap(lambda subkey: jax.random.permutation(subkey, routes_dev))(jax.random.split(key_order, devices_all)).astype(jnp.int32)
    shuffles = shuffles.reshape(N_NODE, N_LOCAL, routes_dev)
    members = jnp.take_along_axis(member_slot, shuffles, axis=2)
    chosen = members[target_node, source_local[:, None], position]
    expert = target_node * EXP_NODE + chosen
    return expert.reshape(TOK_DEV * devices_all, TOP).astype(jnp.int32)


def place_ends(array, own_key, low, largest):
    place = [jax.random.randint(jax.random.fold_in(own_key, axis), (), 0, length) for axis, length in enumerate(array.shape)]
    main_axis = array.shape.index(max(array.shape))
    next_to = place[:main_axis] + [(place[main_axis] + 1) % array.shape[main_axis]] + place[main_axis + 1:]
    return array.at[tuple(place)].set(low).at[tuple(next_to)].set(largest)


def steps_of(rng, dims, cuts, least, high):
    loudness = 1.0
    for dim, blocks in cuts:
        heights = jax.random.uniform(jax.random.fold_in(jax.random.fold_in(rng, 6), dim), (blocks,), jnp.float32, least / len(cuts), high / len(cuts))
        loudness = loudness * jnp.repeat(jnp.exp(heights), dims[dim] // blocks).reshape((-1,) + (1,) * (len(dims) - 1 - dim))
    return loudness


def scatter_about(stream_key, shape, deviation, bound, cuts=(), held_as=jnp.bfloat16):
    entries = deviation * jax.random.normal(stream_key, shape, jnp.float32)
    if cuts:
        entries = entries * steps_of(stream_key, shape, cuts, -0.22, 0.18)
    return jnp.clip(entries, -bound, bound).astype(held_as)


def setup_inputs(seed: int = 0) -> dict:
    seeds = jax.random.split(jax.random.key(seed), 7)
    return {
        "tokens": scatter_about(seeds[0], (TOKENS, D), 1.0, 6.0, ((0, 1024),)),
        "expert_ids": draw_expert_ids(jax.random.fold_in(seeds[6], 71), 0),
        "combine_codes": place_ends(jax.random.randint(seeds[2], (TOKENS, TOP), 1, 17), jax.random.fold_in(seeds[2], 1), 1, 16).astype(jnp.int32),
        "gate_weight": scatter_about(seeds[3], (EXPERTS * SLICES, D, H_DEV), D ** -0.5, 0.09375, ((0, 1024),)),
        "up_weight": scatter_about(seeds[4], (EXPERTS * SLICES, D, H_DEV), D ** -0.5, 0.09375, ((0, 1024),)),
        "down_weight": scatter_about(seeds[5], (EXPERTS * SLICES, H_DEV, D), FF ** -0.5, 0.1875, ((0, 1024),)),
    }


def settle(values):
    return lax.optimization_barrier(values.astype(jnp.bfloat16)).astype(jnp.float32)


def reference(tokens, expert_ids, combine_codes, gate_weight, up_weight, down_weight):
    token_total = tokens.shape[0]
    codes = combine_codes.astype(jnp.float32)
    weights = (codes / jnp.sum(codes, axis=1, keepdims=True)).reshape(-1)
    flat_ids = expert_ids.reshape(-1).astype(jnp.int32)
    order = jnp.argsort(flat_ids, stable=True).astype(jnp.int32)
    counts = jnp.sum((flat_ids[None, :] == jnp.arange(EXPERTS, dtype=jnp.int32)[:, None]).astype(jnp.int32), axis=1)
    starts = (jnp.cumsum(counts) - counts).astype(jnp.int32)
    most = N_LOCAL * EXPERT_CAP
    padded = jnp.concatenate([order, jnp.zeros((most,), jnp.int32)])

    def one_expert(expert, total):
        picked = lax.dynamic_slice_in_dim(padded, starts[expert], most)
        live = jnp.arange(most) < counts[expert]
        owner = jnp.where(live, picked // TOP, token_total).astype(jnp.int32)
        rows = jnp.where(live[:, None], tokens[picked // TOP], 0).astype(jnp.float32)
        first = (expert * SLICES).astype(jnp.int32)
        gate_part = lax.dynamic_slice_in_dim(gate_weight, first, SLICES, 0).astype(jnp.float32)
        up_part = lax.dynamic_slice_in_dim(up_weight, first, SLICES, 0).astype(jnp.float32)
        down_part = lax.dynamic_slice_in_dim(down_weight, first, SLICES, 0).astype(jnp.float32)
        gate = jnp.einsum("rd,sdh->srh", rows, gate_part)
        upper = jnp.einsum("rd,sdh->srh", rows, up_part)
        hidden = settle(jax.nn.silu(gate) * upper)
        partial_out = settle(jnp.einsum("srh,shd->srd", hidden, down_part))
        expert_out = settle(jnp.sum(partial_out, axis=0))
        return total.at[owner].add(weights[picked][:, None] * expert_out)

    total = lax.fori_loop(0, EXPERTS, one_expert, jnp.zeros((token_total + 1, D), jnp.float32))
    return total[:token_total].astype(jnp.bfloat16)
```

```python
import functools

import jax
import jax.numpy as jnp
from jax import lax
from jax.experimental import pallas as pl
from jax.experimental.pallas import tpu as pltpu
from jax.sharding import Mesh
from jax.sharding import PartitionSpec as P

TOP = 4
MEMBERS = 4
CAP = 16
LANES = 128
NODE = ("z", "core")
LOCAL = ("x", "y")
ALL = ("z", "core", "y", "x")
f32, bf16, i32 = jnp.float32, jnp.bfloat16, jnp.int32
VMEM = pl.BlockSpec(memory_space=pltpu.VMEM)
SMEM = pl.BlockSpec(memory_space=pltpu.SMEM)


def exchange(value, axes):
    return lax.all_to_all(value, axes, split_axis=0, concat_axis=0, tiled=True)


def shift(value, by, count):
    return lax.ppermute(value, "x", [(i, (i + by) % count) for i in range(count)])


def mix_kernel(ids_ref, codes_ref, mix_ref):
    codes = codes_ref[...].astype(f32)
    weights = codes / jnp.sum(codes, axis=0, keepdims=True)
    target = ids_ref[...] // MEMBERS
    node = lax.broadcasted_iota(i32, mix_ref.shape, 0)
    mix = jnp.zeros(mix_ref.shape, f32)
    for k in range(TOP):
        mix = mix + jnp.where(target[k : k + 1, :] == node, weights[k : k + 1, :], 0.0)
    mix_ref[...] = mix


def spread_kernel(slot_ref, spread_ref):
    row = lax.broadcasted_iota(i32, spread_ref.shape, 0)
    pair = spread_ref.shape[0] // (MEMBERS * CAP)
    wanted = row // (pair * CAP) * CAP + row % CAP
    spread_ref[...] = jnp.where(wanted == slot_ref[...], 1.0, 0.0).astype(bf16)


def share_kernel(xs, x_ref, rows_ref, *refs):
    weights, out_ref = refs[:-1], refs[-1]
    x = x_ref[0]
    per = out_ref.shape[0] // xs
    for k in range(xs):
        source = lax.rem(x - k + xs, xs)
        gate_at = pl.multiple_of(source * LANES, LANES)
        up_at = pl.multiple_of((source + xs) * LANES, LANES)
        for q in range(xs):
            part = jnp.dot(
                rows_ref[q * per : (q + 1) * per, :], weights[k][...], preferred_element_type=f32
            ).astype(bf16)
            out_ref[q * per : (q + 1) * per, pl.ds(gate_at, LANES)] = part[:, :LANES]
            out_ref[q * per : (q + 1) * per, pl.ds(up_at, LANES)] = part[:, LANES:]


def down_kernel(xs, x_ref, share_ref, w0_ref, w1_ref, w3_ref, w2a_ref, w2b_ref, out_ref, hid_ref):
    x = x_ref[0]
    both = share_ref[0].astype(f32)
    for q in range(1, xs):
        both = both + share_ref[q].astype(f32)
    units = xs * LANES
    hid_ref[...] = (jax.nn.silu(both[:, :units]) * both[:, units:]).astype(bf16)
    mine = [
        hid_ref[:, pl.ds(pl.multiple_of(lax.rem(x - k + xs, xs) * LANES, LANES), LANES)]
        for k in range(xs)
    ]
    half = LANES // 2
    step = 512
    for n in range(0, out_ref.shape[1], step):
        cols = slice(n, n + step)
        total = jnp.dot(mine[0], w0_ref[:, cols], preferred_element_type=f32)
        total += jnp.dot(mine[1], w1_ref[:, cols], preferred_element_type=f32)
        total += jnp.dot(mine[3], w3_ref[:, cols], preferred_element_type=f32)
        total += jnp.dot(mine[2][:, :half], w2a_ref[:, cols], preferred_element_type=f32)
        total += jnp.dot(mine[2][:, half:], w2b_ref[:, cols], preferred_element_type=f32)
        out_ref[:, cols] = total.astype(bf16)


def body(tokens, expert_ids, combine_codes, gate_weight, up_weight, down_weight):
    nodes = lax.axis_size("z") * lax.axis_size("core")
    ys, xs = lax.axis_size("y"), lax.axis_size("x")
    pair = ys // MEMBERS
    token_count, width = tokens.shape
    chunk = width // xs
    units = gate_weight.shape[2]
    x = lax.axis_index("x")
    x_arg = x.astype(i32)[None]

    target = expert_ids // MEMBERS
    member = expert_ids % MEMBERS
    named = target[None, :, :] == jnp.arange(nodes, dtype=i32)[:, None, None]
    pick = jnp.any(named, axis=2).astype(bf16)
    slot_member = jnp.sum(jnp.where(named, member[None], 0), axis=(1, 2))
    outgoing = jnp.dot(pick, tokens, preferred_element_type=f32).astype(bf16)
    tag = jnp.broadcast_to(slot_member.astype(bf16)[:, None, None], (nodes, 4, LANES))
    outgoing = jnp.concatenate([outgoing.reshape(nodes, width // LANES, LANES), tag], axis=1)
    arrived = exchange(outgoing, NODE)
    arrived_member = arrived[:, -1, 0].astype(i32)
    arrived = arrived[:, : width // LANES].reshape(nodes, width)

    mix = pl.pallas_call(
        mix_kernel,
        out_shape=jax.ShapeDtypeStruct((nodes, token_count), f32),
        in_specs=[VMEM, VMEM],
        out_specs=VMEM,
        compiler_params=pltpu.CompilerParams(vmem_limit_bytes=1 << 20),
    )(expert_ids.T, combine_codes.T)

    joined = jnp.concatenate([gate_weight[0], up_weight[0]], axis=1)
    blocks = []
    for k in range(xs):
        block = lax.dynamic_slice_in_dim(joined, lax.rem(x + k, xs) * chunk, chunk, 0)
        blocks.append(shift(block, k, xs) if k else block)
    down = down_weight[0]
    down_left = shift(down, 1, xs)
    down_right = shift(down, xs - 1, xs)
    half = units // 2
    down_far_a = shift(down_left[:half], 1, xs)
    down_far_b = shift(down_right[half:], xs - 1, xs)

    marks = arrived_member[:, None] == jnp.arange(MEMBERS, dtype=i32)[None, :]
    counts = marks.astype(i32)
    rank = jnp.sum((jnp.cumsum(counts, axis=0) - counts) * counts, axis=1)
    place_slot = arrived_member * CAP + rank
    place = (place_slot[None, :] == jnp.arange(MEMBERS * CAP, dtype=i32)[:, None]).astype(bf16)
    bundle = jnp.dot(place, arrived, preferred_element_type=f32).astype(bf16)
    bundle = bundle.reshape(MEMBERS, 1, CAP, xs, chunk).transpose(3, 0, 1, 2, 4)
    bundle = jnp.broadcast_to(bundle, (xs, MEMBERS, pair, CAP, chunk)).reshape(xs * ys, CAP, chunk)
    spread = pl.pallas_call(
        spread_kernel,
        out_shape=jax.ShapeDtypeStruct((ys * CAP, nodes), bf16),
        in_specs=[VMEM],
        out_specs=VMEM,
        compiler_params=pltpu.CompilerParams(vmem_limit_bytes=1 << 20),
    )(place_slot[None, :])
    rows = exchange(bundle, LOCAL).reshape(xs * ys * CAP, chunk)

    share = pl.pallas_call(
        functools.partial(share_kernel, xs),
        out_shape=jax.ShapeDtypeStruct((xs * ys * CAP, 2 * xs * units), bf16),
        in_specs=[SMEM] + [VMEM] * (1 + xs),
        out_specs=VMEM,
        compiler_params=pltpu.CompilerParams(vmem_limit_bytes=12 << 20),
        cost_estimate=pl.CostEstimate(flops=2 << 30, bytes_accessed=4 << 20, transcendentals=0),
    )(x_arg, rows, *blocks)
    share = exchange(share.reshape(xs, ys * CAP, 2 * xs * units), "x")
    partial_out = pl.pallas_call(
        functools.partial(down_kernel, xs),
        out_shape=jax.ShapeDtypeStruct((ys * CAP, width), bf16),
        in_specs=[SMEM] + [VMEM] * 6,
        out_specs=VMEM,
        scratch_shapes=[pltpu.VMEM((ys * CAP, xs * units), bf16)],
        compiler_params=pltpu.CompilerParams(vmem_limit_bytes=16 << 20),
        cost_estimate=pl.CostEstimate(flops=1 << 30, bytes_accessed=6 << 20, transcendentals=1 << 16),
    )(x_arg, share, down, down_left, down_right, down_far_a, down_far_b)
    returned = exchange(partial_out.reshape(ys, CAP, width), "y").reshape(ys * CAP, width)

    results = jnp.dot(spread.T, returned, preferred_element_type=f32).astype(bf16)
    home = exchange(results.reshape(nodes, width // LANES, LANES), NODE).reshape(nodes, width)

    mixed = lax.dot(mix.T, home.astype(f32), precision=lax.Precision.HIGHEST)
    return mixed.astype(bf16)


def solution(mesh):
    nodes, locals_ = mesh.shape["node"], mesh.shape["local"]
    split = Mesh(mesh.devices.reshape(nodes // 2, 2, locals_ // 4, 4), ALL)
    in_specs = (
        P(ALL, None),
        P(ALL, None),
        P(ALL, None),
        P(ALL, None, None),
        P(ALL, None, None),
        P(ALL, None, None),
    )

    return jax.shard_map(body, mesh=split, in_specs=in_specs, out_specs=P(ALL, None), check_vma=False)
```

```python
import functools

import jax
import jax.numpy as jnp
from jax import lax
from jax.experimental import pallas as pl
from jax.experimental.pallas import tpu as pltpu
from jax.sharding import Mesh
from jax.sharding import PartitionSpec as P

TOP = 4
MEMBERS = 4
CAP = 16
LANES = 128
NODE = ("z", "core")
LOCAL = ("x", "y")
ALL = ("z", "core", "y", "x")
f32, bf16, i32 = jnp.float32, jnp.bfloat16, jnp.int32
VMEM = pl.BlockSpec(memory_space=pltpu.VMEM)
SMEM = pl.BlockSpec(memory_space=pltpu.SMEM)
HBM = pl.BlockSpec(memory_space=pltpu.HBM)
ANY = pl.BlockSpec(memory_space=pl.ANY)


def exchange(value, axes):
    return lax.all_to_all(value, axes, split_axis=0, concat_axis=0, tiled=True)


def shift(value, by, count):
    return lax.ppermute(value, "x", [(i, (i + by) % count) for i in range(count)])


def weight_kernel(codes_ref, out_ref):
    codes = codes_ref[...].astype(f32)
    out_ref[...] = codes / jnp.sum(codes, axis=0, keepdims=True)


def target_kernel(ids_ref, out_ref):
    out_ref[...] = ids_ref[...] // MEMBERS


def mix_kernel(target_ref, weights_ref, mix_ref):
    node = lax.broadcasted_iota(i32, mix_ref.shape, 0)
    mix = jnp.zeros(mix_ref.shape, f32)
    for k in range(TOP):
        mix = mix + jnp.where(target_ref[k : k + 1, :] == node, weights_ref[k : k + 1, :], 0.0)
    mix_ref[...] = mix


def split_kernel(mix_ref, out_ref):
    high = mix_ref[...].astype(bf16)
    out_ref[:, : mix_ref.shape[1]] = high
    out_ref[:, mix_ref.shape[1] :] = (mix_ref[...] - high.astype(f32)).astype(bf16)


def slot_kernel(tag_ref, place_ref, spread_ref):
    tag = tag_ref[:, tag_ref.shape[1] - 1, :].astype(f32)
    nodes = tag.shape[0]
    row = lax.broadcasted_iota(i32, (nodes, nodes), 0)
    column = lax.broadcasted_iota(i32, (nodes, nodes), 1)
    earlier = jnp.where(column < row, 1.0, 0.0).astype(bf16)
    slot = tag * CAP
    for m in range(MEMBERS):
        mark = jnp.where(tag == m, 1.0, 0.0)
        slot = slot + mark * jnp.dot(earlier, mark.astype(bf16), preferred_element_type=f32)
    lane = lax.broadcasted_iota(i32, spread_ref.shape, 1)
    pair = spread_ref.shape[1] // (MEMBERS * CAP)
    wanted = lane // (pair * CAP) * CAP + lane % CAP
    spread_ref[...] = jnp.where(slot == wanted.astype(f32), 1.0, 0.0).astype(bf16)
    place = jnp.where(slot == lane.astype(f32), 1.0, 0.0).astype(bf16)
    place_ref[...] = place[:, : place_ref.shape[1]]


def share_kernel(xs, x_ref, rows_ref, gate_ref, up_ref, *refs):
    others, (out_ref, rows, weights, out, row_sem, weight_sem, out_sem) = refs[: xs - 1], refs[xs - 1 :]
    x = x_ref[0]
    depth = weights.shape[1]
    mine = pl.ds(pl.multiple_of(x * depth, depth), depth)
    parts = 2
    per = out_ref.shape[0] // parts
    takes = [
        pltpu.make_async_copy(
            rows_ref.at[q * per : (q + 1) * per], rows.at[q * per : (q + 1) * per], row_sem.at[q]
        )
        for q in range(parts)
    ]
    loads = [[pltpu.make_async_copy(ref, weights.at[k + 1], weight_sem.at[k])] for k, ref in enumerate(others)]
    loads.append(
        [
            pltpu.make_async_copy(
                ref.at[0, mine], weights.at[0, :, i * LANES : (i + 1) * LANES], weight_sem.at[xs - 1 + i]
            )
            for i, ref in enumerate((gate_ref, up_ref))
        ]
    )
    takes[0].start()
    for load in loads:
        for copy in load:
            copy.start()
    takes[1].start()
    sends = []
    for q in range(parts):
        at = slice(q * per, (q + 1) * per)
        takes[q].wait()
        for load, k in zip(loads, (*range(1, xs), 0)):
            if q == 0:
                for copy in load:
                    copy.wait()
            source = lax.rem(x - k + xs, xs)
            gate_at = pl.multiple_of(source * LANES, LANES)
            up_at = pl.multiple_of((source + xs) * LANES, LANES)
            part = jnp.dot(rows[at, :], weights[k], preferred_element_type=f32).astype(bf16)
            out[at, pl.ds(gate_at, LANES)] = part[:, :LANES]
            out[at, pl.ds(up_at, LANES)] = part[:, LANES:]
        send = pltpu.make_async_copy(out.at[at], out_ref.at[at], out_sem.at[q])
        send.start()
        sends.append(send)
    for send in sends:
        send.wait()


def down_kernel(xs, step, x_ref, share_ref, w0_ref, w1_ref, w3_ref, w2a_ref, w2b_ref, out_ref, share, hid, weights, out, share_sem, weight_sem, out_sem):
    width = out_ref.shape[1]
    half = LANES // 2
    parts = 2
    take = pltpu.make_async_copy(share_ref, share, share_sem)
    take.start()
    loads = []
    for c in range(parts):
        cols = slice(c * (width // parts), (c + 1) * (width // parts))
        pieces = (
            (w0_ref, weights.at[0]),
            (w1_ref, weights.at[1]),
            (w3_ref, weights.at[3]),
            (w2a_ref, weights.at[2, :half]),
            (w2b_ref, weights.at[2, half:]),
        )
        load = [
            pltpu.make_async_copy(a.at[:, cols], b.at[:, cols], weight_sem.at[c * len(pieces) + i])
            for i, (a, b) in enumerate(pieces)
        ]
        for copy in load:
            copy.start()
        loads.append(load)
    x = x_ref[0]
    take.wait()
    both = share[0].astype(f32)
    for q in range(1, xs):
        both = both + share[q].astype(f32)
    units = xs * LANES
    hid[...] = (jax.nn.silu(both[:, :units]) * both[:, units:]).astype(bf16)
    mine = [
        hid[:, pl.ds(pl.multiple_of(lax.rem(x - k + xs, xs) * LANES, LANES), LANES)]
        for k in range(xs)
    ]
    sends = []
    for i, n in enumerate(range(0, width, step)):
        if n % (width // parts) == 0:
            for copy in loads[n // (width // parts)]:
                copy.wait()
        cols = slice(n, n + step)
        total = jnp.dot(mine[0], weights[0, :, cols], preferred_element_type=f32)
        for k in range(1, xs):
            total += jnp.dot(mine[k], weights[k, :, cols], preferred_element_type=f32)
        out[:, cols] = total.astype(bf16)
        send = pltpu.make_async_copy(out.at[:, cols], out_ref.at[:, cols], out_sem.at[i])
        send.start()
        sends.append(send)
    for send in sends:
        send.wait()


def held(arrays):
    return [pltpu.with_memory_space_constraint(a, pltpu.HBM) for a in arrays]


def small(kernel, shapes, *args, in_specs=None):
    many = isinstance(shapes, (tuple, list))
    return pl.pallas_call(
        kernel,
        out_shape=shapes,
        in_specs=in_specs or [VMEM] * len(args),
        out_specs=[VMEM] * len(shapes) if many else VMEM,
        compiler_params=pltpu.CompilerParams(vmem_limit_bytes=1 << 20),
    )(*args)


def body(tokens, expert_ids, combine_codes, gate_weight, up_weight, down_weight):
    nodes = lax.axis_size("z") * lax.axis_size("core")
    ys, xs = lax.axis_size("y"), lax.axis_size("x")
    pair = ys // MEMBERS
    token_count, width = tokens.shape
    chunk = width // xs
    units = gate_weight.shape[2]
    x = lax.axis_index("x")
    x_arg = x.astype(i32)[None]

    target = expert_ids // MEMBERS
    member = expert_ids % MEMBERS
    named = target[None, :, :] == jnp.arange(nodes, dtype=i32)[:, None, None]
    pick = jnp.any(named, axis=2).astype(bf16)
    slot_member = jnp.sum(jnp.where(named, member[None], 0), axis=(1, 2))
    outgoing = jnp.dot(pick, tokens, preferred_element_type=f32).astype(bf16)
    tag = jnp.broadcast_to(slot_member.astype(bf16)[:, None, None], (nodes, 4, LANES))
    outgoing = jnp.concatenate([outgoing.reshape(nodes, width // LANES, LANES), tag], axis=1)
    arrived = exchange(outgoing, NODE)
    weights = small(weight_kernel, jax.ShapeDtypeStruct((TOP, token_count), f32), combine_codes.T)

    joined = jnp.concatenate([gate_weight[0], up_weight[0]], axis=1)
    blocks = []
    for k in range(1, xs):
        block = lax.dynamic_slice_in_dim(joined, lax.rem(x + k, xs) * chunk, chunk, 0)
        blocks.append(shift(block, k, xs))
    down = down_weight[0]
    down_left = shift(down, 1, xs)
    down_right = shift(down, xs - 1, xs)
    half = units // 2
    down_far_a = shift(down_left[:half], 1, xs)
    down_far_b = shift(down_right[half:], xs - 1, xs)

    place, spread = pl.pallas_call(
        slot_kernel,
        grid=(1,),
        out_shape=(
            jax.ShapeDtypeStruct((nodes, MEMBERS * CAP), bf16),
            jax.ShapeDtypeStruct((nodes, ys * CAP), bf16),
        ),
        in_specs=[pl.BlockSpec((nodes, 8, LANES), lambda i: (0, arrived.shape[1] // 8 - 1, 0))],
        out_specs=(
            pl.BlockSpec((nodes, MEMBERS * CAP), lambda i: (0, 0)),
            pl.BlockSpec((nodes, ys * CAP), lambda i: (0, 0)),
        ),
        compiler_params=pltpu.CompilerParams(vmem_limit_bytes=1 << 20),
    )(arrived)
    arrived = arrived[:, : width // LANES].reshape(nodes, width)
    bundle = jnp.dot(place.T, arrived, preferred_element_type=f32).astype(bf16)
    bundle = bundle.reshape(MEMBERS, 1, CAP, xs, chunk).transpose(3, 0, 1, 2, 4)
    bundle = jnp.broadcast_to(bundle, (xs, MEMBERS, pair, CAP, chunk)).reshape(xs * ys, CAP, chunk)
    target = small(target_kernel, jax.ShapeDtypeStruct((TOP, token_count), i32), expert_ids.T)
    rows = exchange(bundle, LOCAL).reshape(xs * ys * CAP, chunk)

    share_shape = (xs * ys * CAP, 2 * xs * units)
    share = pl.pallas_call(
        functools.partial(share_kernel, xs),
        out_shape=pltpu.HBM(share_shape, bf16),
        in_specs=[SMEM, ANY] + [HBM] * (1 + xs),
        out_specs=HBM,
        scratch_shapes=[
            pltpu.VMEM((xs * ys * CAP, chunk), bf16),
            pltpu.VMEM((xs, chunk, 2 * units), bf16),
            pltpu.VMEM(share_shape, bf16),
            pltpu.SemaphoreType.DMA((2,)),
            pltpu.SemaphoreType.DMA((xs + 1,)),
            pltpu.SemaphoreType.DMA((2,)),
        ],
        compiler_params=pltpu.CompilerParams(vmem_limit_bytes=20 << 20),
        cost_estimate=pl.CostEstimate(flops=2 << 30, bytes_accessed=4 << 20, transcendentals=0),
    )(x_arg, rows, *held((gate_weight, up_weight, *blocks)))
    share = exchange(share.reshape(xs, ys * CAP, 2 * xs * units), "x")
    step = 256
    out_shape = (ys * CAP, width)
    partial_out = pl.pallas_call(
        functools.partial(down_kernel, xs, step),
        out_shape=pltpu.HBM(out_shape, bf16),
        in_specs=[SMEM, ANY] + [HBM] * 5,
        out_specs=HBM,
        scratch_shapes=[
            pltpu.VMEM((xs, ys * CAP, 2 * xs * units), bf16),
            pltpu.VMEM((ys * CAP, xs * units), bf16),
            pltpu.VMEM((xs, units, width), bf16),
            pltpu.VMEM(out_shape, bf16),
            pltpu.SemaphoreType.DMA(()),
            pltpu.SemaphoreType.DMA((10,)),
            pltpu.SemaphoreType.DMA((width // step,)),
        ],
        compiler_params=pltpu.CompilerParams(vmem_limit_bytes=20 << 20),
        cost_estimate=pl.CostEstimate(flops=1 << 30, bytes_accessed=6 << 20, transcendentals=1 << 16),
    )(x_arg, share, *held((down, down_left, down_right, down_far_a, down_far_b)))
    mix = small(
        mix_kernel, jax.ShapeDtypeStruct((nodes, token_count), f32), target, weights
    )
    returned = exchange(partial_out.reshape(ys, CAP, width), "y").reshape(ys * CAP, width)

    results = jnp.dot(spread, returned, preferred_element_type=f32).astype(bf16)
    terms = small(split_kernel, jax.ShapeDtypeStruct((nodes, 2 * token_count), bf16), mix)
    home = exchange(results.reshape(nodes, width // LANES, LANES), NODE).reshape(nodes, width)
    mixed = jnp.dot(terms.T, home, preferred_element_type=f32)
    return (mixed[:token_count] + mixed[token_count:]).astype(bf16)


def solution(mesh):
    nodes, locals_ = mesh.shape["node"], mesh.shape["local"]
    split = Mesh(mesh.devices.reshape(nodes // 2, 2, locals_ // 4, 4), ALL)
    in_specs = (
        P(ALL, None),
        P(ALL, None),
        P(ALL, None),
        P(ALL, None, None),
        P(ALL, None, None),
        P(ALL, None, None),
    )

    return jax.shard_map(body, mesh=split, in_specs=in_specs, out_specs=P(ALL, None), check_vma=False)
```

```python
import functools

import jax
import jax.numpy as jnp
from jax import lax
from jax.experimental import pallas as pl
from jax.experimental.pallas import tpu as pltpu
from jax.sharding import Mesh
from jax.sharding import PartitionSpec as P

TOP = 4
MEMBERS = 4
CAP = 16
LANES = 128
NODE = ("z", "core")
LOCAL = ("x", "y")
ALL = ("z", "core", "y", "x")
f32, bf16, i32 = jnp.float32, jnp.bfloat16, jnp.int32
VMEM = pl.BlockSpec(memory_space=pltpu.VMEM)
SMEM = pl.BlockSpec(memory_space=pltpu.SMEM)
HBM = pl.BlockSpec(memory_space=pltpu.HBM)
ANY = pl.BlockSpec(memory_space=pl.ANY)


def exchange(value, axes):
    return lax.all_to_all(value, axes, split_axis=0, concat_axis=0, tiled=True)


def shift(value, by, count):
    return lax.ppermute(value, "x", [(i, (i + by) % count) for i in range(count)])


def weight_kernel(codes_ref, out_ref):
    codes = codes_ref[...].astype(f32)
    out_ref[...] = codes / jnp.sum(codes, axis=0, keepdims=True)


def target_kernel(ids_ref, out_ref):
    out_ref[...] = ids_ref[...] // MEMBERS


def mix_kernel(target_ref, weights_ref, out_ref):
    tokens = target_ref.shape[1]
    node = lax.broadcasted_iota(i32, (out_ref.shape[0], tokens), 0)
    mix = jnp.zeros(node.shape, f32)
    for k in range(TOP):
        mix = mix + jnp.where(target_ref[k : k + 1, :] == node, weights_ref[k : k + 1, :], 0.0)
    high = mix.astype(bf16)
    out_ref[:, :tokens] = high
    out_ref[:, tokens:] = (mix - high.astype(f32)).astype(bf16)


def slot_kernel(tag_ref, place_ref, spread_ref):
    tag = tag_ref[:, tag_ref.shape[1] - 1, :].astype(f32)
    nodes = tag.shape[0]
    row = lax.broadcasted_iota(i32, (nodes, nodes), 0)
    column = lax.broadcasted_iota(i32, (nodes, nodes), 1)
    earlier = jnp.where(column < row, 1.0, 0.0).astype(bf16)
    slot = tag * CAP
    for m in range(MEMBERS):
        mark = jnp.where(tag == m, 1.0, 0.0)
        slot = slot + mark * jnp.dot(earlier, mark.astype(bf16), preferred_element_type=f32)
    lane = lax.broadcasted_iota(i32, spread_ref.shape, 1)
    pair = spread_ref.shape[1] // (MEMBERS * CAP)
    wanted = lane // (pair * CAP) * CAP + lane % CAP
    spread_ref[...] = jnp.where(slot == wanted.astype(f32), 1.0, 0.0).astype(bf16)
    place = jnp.where(slot == lane.astype(f32), 1.0, 0.0).astype(bf16)
    place_ref[...] = place[:, : place_ref.shape[1]]


def share_kernel(xs, x_ref, rows_ref, gate_ref, up_ref, *refs):
    others, (out_ref, rows, weights, out, row_sem, weight_sem, out_sem) = refs[: xs - 1], refs[xs - 1 :]
    x = x_ref[0]
    depth = weights.shape[1]
    mine = pl.ds(pl.multiple_of(x * depth, depth), depth)
    parts = 2
    per = out_ref.shape[0] // parts
    takes = [
        pltpu.make_async_copy(
            rows_ref.at[q * per : (q + 1) * per], rows.at[q * per : (q + 1) * per], row_sem.at[q]
        )
        for q in range(parts)
    ]
    loads = [[pltpu.make_async_copy(ref, weights.at[k + 1], weight_sem.at[k])] for k, ref in enumerate(others)]
    loads.append(
        [
            pltpu.make_async_copy(
                ref.at[0, mine], weights.at[0, :, i * LANES : (i + 1) * LANES], weight_sem.at[xs - 1 + i]
            )
            for i, ref in enumerate((gate_ref, up_ref))
        ]
    )
    takes[0].start()
    for load in loads:
        for copy in load:
            copy.start()
    takes[1].start()
    sends = []
    for q in range(parts):
        at = slice(q * per, (q + 1) * per)
        takes[q].wait()
        for load, k in zip(loads, (*range(1, xs), 0)):
            if q == 0:
                for copy in load:
                    copy.wait()
            source = lax.rem(x - k + xs, xs)
            gate_at = pl.multiple_of(source * LANES, LANES)
            up_at = pl.multiple_of((source + xs) * LANES, LANES)
            part = jnp.dot(rows[at, :], weights[k], preferred_element_type=f32).astype(bf16)
            out[at, pl.ds(gate_at, LANES)] = part[:, :LANES]
            out[at, pl.ds(up_at, LANES)] = part[:, LANES:]
        send = pltpu.make_async_copy(out.at[at], out_ref.at[at], out_sem.at[q])
        send.start()
        sends.append(send)
    for send in sends:
        send.wait()


def down_kernel(xs, x_ref, share_ref, w0_ref, w1_ref, w3_ref, w2a_ref, w2b_ref, out_ref, hid_ref):
    x = x_ref[0]
    both = share_ref[0].astype(f32)
    for q in range(1, xs):
        both = both + share_ref[q].astype(f32)
    units = xs * LANES
    hid_ref[...] = (jax.nn.silu(both[:, :units]) * both[:, units:]).astype(bf16)
    mine = [
        hid_ref[:, pl.ds(pl.multiple_of(lax.rem(x - k + xs, xs) * LANES, LANES), LANES)]
        for k in range(xs)
    ]
    half = LANES // 2
    step = 512
    for n in range(0, out_ref.shape[1], step):
        cols = slice(n, n + step)
        total = jnp.dot(mine[0], w0_ref[:, cols], preferred_element_type=f32)
        total += jnp.dot(mine[1], w1_ref[:, cols], preferred_element_type=f32)
        total += jnp.dot(mine[3], w3_ref[:, cols], preferred_element_type=f32)
        total += jnp.dot(mine[2][:, :half], w2a_ref[:, cols], preferred_element_type=f32)
        total += jnp.dot(mine[2][:, half:], w2b_ref[:, cols], preferred_element_type=f32)
        out_ref[:, cols] = total.astype(bf16)


def held(arrays):
    return [pltpu.with_memory_space_constraint(a, pltpu.HBM) for a in arrays]


def small(kernel, shapes, *args, in_specs=None):
    many = isinstance(shapes, (tuple, list))
    return pl.pallas_call(
        kernel,
        out_shape=shapes,
        in_specs=in_specs or [VMEM] * len(args),
        out_specs=[VMEM] * len(shapes) if many else VMEM,
        compiler_params=pltpu.CompilerParams(vmem_limit_bytes=1 << 20),
    )(*args)


def body(tokens, expert_ids, combine_codes, gate_weight, up_weight, down_weight):
    nodes = lax.axis_size("z") * lax.axis_size("core")
    ys, xs = lax.axis_size("y"), lax.axis_size("x")
    pair = ys // MEMBERS
    token_count, width = tokens.shape
    chunk = width // xs
    units = gate_weight.shape[2]
    x = lax.axis_index("x")
    x_arg = x.astype(i32)[None]

    target = expert_ids // MEMBERS
    member = expert_ids % MEMBERS
    named = target[None, :, :] == jnp.arange(nodes, dtype=i32)[:, None, None]
    pick = jnp.any(named, axis=2).astype(bf16)
    slot_member = jnp.sum(jnp.where(named, member[None], 0), axis=(1, 2))
    outgoing = jnp.dot(pick, tokens, preferred_element_type=f32).astype(bf16)
    tag = jnp.broadcast_to(slot_member.astype(bf16)[:, None, None], (nodes, xs, LANES))
    outgoing = jnp.concatenate([outgoing.reshape(nodes, xs, chunk), tag], axis=2)
    arrived = exchange(outgoing, NODE)
    weights = small(
        weight_kernel, jax.ShapeDtypeStruct((TOP, token_count), f32), combine_codes.T
    )

    joined = jnp.concatenate([gate_weight[0], up_weight[0]], axis=1)
    blocks = []
    for k in range(1, xs):
        block = lax.dynamic_slice_in_dim(joined, lax.rem(x + k, xs) * chunk, chunk, 0)
        blocks.append(shift(block, k, xs))
    down = down_weight[0]
    down_left = shift(down, 1, xs)
    down_right = shift(down, xs - 1, xs)
    half = units // 2
    down_far_a = shift(down_left[:half], 1, xs)
    down_far_b = shift(down_right[half:], xs - 1, xs)

    place, spread = pl.pallas_call(
        slot_kernel,
        grid=(1,),
        out_shape=(
            jax.ShapeDtypeStruct((nodes, MEMBERS * CAP), bf16),
            jax.ShapeDtypeStruct((nodes, ys * CAP), bf16),
        ),
        in_specs=[pl.BlockSpec((nodes, xs, LANES), lambda i: (0, 0, chunk // LANES))],
        out_specs=(
            pl.BlockSpec((nodes, MEMBERS * CAP), lambda i: (0, 0)),
            pl.BlockSpec((nodes, ys * CAP), lambda i: (0, 0)),
        ),
        compiler_params=pltpu.CompilerParams(vmem_limit_bytes=1 << 20),
    )(arrived)
    bundle = jnp.dot(place.T, arrived.reshape(nodes, -1), preferred_element_type=f32).astype(bf16)
    bundle = bundle.reshape(MEMBERS, 1, CAP, xs, chunk + LANES)[..., :chunk].transpose(3, 0, 1, 2, 4)
    bundle = jnp.broadcast_to(bundle, (xs, MEMBERS, pair, CAP, chunk)).reshape(xs * ys, CAP, chunk)
    target = small(target_kernel, jax.ShapeDtypeStruct((TOP, token_count), i32), expert_ids.T)
    rows = exchange(bundle, LOCAL).reshape(xs * ys * CAP, chunk)

    share_shape = (xs * ys * CAP, 2 * xs * units)
    share = pl.pallas_call(
        functools.partial(share_kernel, xs),
        out_shape=pltpu.HBM(share_shape, bf16),
        in_specs=[SMEM, ANY] + [HBM] * (1 + xs),
        out_specs=HBM,
        scratch_shapes=[
            pltpu.VMEM((xs * ys * CAP, chunk), bf16),
            pltpu.VMEM((xs, chunk, 2 * units), bf16),
            pltpu.VMEM(share_shape, bf16),
            pltpu.SemaphoreType.DMA((2,)),
            pltpu.SemaphoreType.DMA((xs + 1,)),
            pltpu.SemaphoreType.DMA((2,)),
        ],
        compiler_params=pltpu.CompilerParams(vmem_limit_bytes=20 << 20),
        cost_estimate=pl.CostEstimate(flops=2 << 30, bytes_accessed=4 << 20, transcendentals=0),
    )(x_arg, rows, *held((gate_weight, up_weight, *blocks)))
    share = exchange(share.reshape(xs, ys * CAP, 2 * xs * units), "x")
    partial_out = pl.pallas_call(
        functools.partial(down_kernel, xs),
        out_shape=jax.ShapeDtypeStruct((ys * CAP, width), bf16),
        in_specs=[SMEM] + [VMEM] * 6,
        out_specs=VMEM,
        scratch_shapes=[pltpu.VMEM((ys * CAP, xs * units), bf16)],
        compiler_params=pltpu.CompilerParams(vmem_limit_bytes=16 << 20),
        cost_estimate=pl.CostEstimate(flops=1 << 30, bytes_accessed=6 << 20, transcendentals=1 << 16),
    )(x_arg, share, down, down_left, down_right, down_far_a, down_far_b)
    returned = exchange(partial_out.reshape(ys, CAP, width), "y").reshape(ys * CAP, width)

    results = jnp.dot(spread, returned, preferred_element_type=f32).astype(bf16)
    terms = small(
        mix_kernel, jax.ShapeDtypeStruct((nodes, 2 * token_count), bf16), target, weights
    )
    home = exchange(results.reshape(nodes, xs, chunk), NODE).reshape(nodes, width)
    mixed = jnp.dot(terms.T, home, preferred_element_type=f32)
    return (mixed[:token_count] + mixed[token_count:]).astype(bf16)


def solution(mesh):
    nodes, locals_ = mesh.shape["node"], mesh.shape["local"]
    split = Mesh(mesh.devices.reshape(nodes // 2, 2, locals_ // 4, 4), ALL)
    in_specs = (
        P(ALL, None),
        P(ALL, None),
        P(ALL, None),
        P(ALL, None, None),
        P(ALL, None, None),
        P(ALL, None, None),
    )

    return jax.shard_map(body, mesh=split, in_specs=in_specs, out_specs=P(ALL, None), check_vma=False)
```

```python
import functools

import jax
import jax.numpy as jnp
from jax import lax
from jax.experimental import pallas as pl
from jax.experimental.pallas import tpu as pltpu
from jax.sharding import Mesh
from jax.sharding import PartitionSpec as P

TOP = 4
MEMBERS = 4
CAP = 16
LANES = 128
NODE = ("z", "core")
LOCAL = ("x", "y")
ALL = ("z", "core", "y", "x")
f32, bf16, i32 = jnp.float32, jnp.bfloat16, jnp.int32
VMEM = pl.BlockSpec(memory_space=pltpu.VMEM)
SMEM = pl.BlockSpec(memory_space=pltpu.SMEM)
HBM = pl.BlockSpec(memory_space=pltpu.HBM)
ANY = pl.BlockSpec(memory_space=pl.ANY)


def exchange(value, axes):
    return lax.all_to_all(value, axes, split_axis=0, concat_axis=0, tiled=True)


def shift(value, by, count):
    return lax.ppermute(value, "x", [(i, (i + by) % count) for i in range(count)])


def weight_kernel(codes_ref, out_ref):
    codes = codes_ref[...].astype(f32)
    out_ref[...] = codes / jnp.sum(codes, axis=0, keepdims=True)


def target_kernel(ids_ref, out_ref):
    out_ref[...] = ids_ref[...] // MEMBERS


def mix_kernel(target_ref, weights_ref, out_ref):
    tokens = target_ref.shape[1]
    node = lax.broadcasted_iota(i32, (out_ref.shape[0], tokens), 0)
    mix = jnp.zeros(node.shape, f32)
    for k in range(TOP):
        mix = mix + jnp.where(target_ref[k : k + 1, :] == node, weights_ref[k : k + 1, :], 0.0)
    high = mix.astype(bf16)
    out_ref[:, :tokens] = high
    out_ref[:, tokens:] = (mix - high.astype(f32)).astype(bf16)


def slot_kernel(tag_ref, place_ref, spread_ref):
    tag = tag_ref[:, tag_ref.shape[1] - 1, :].astype(f32)
    nodes = tag.shape[0]
    row = lax.broadcasted_iota(i32, (nodes, nodes), 0)
    column = lax.broadcasted_iota(i32, (nodes, nodes), 1)
    earlier = jnp.where(column < row, 1.0, 0.0).astype(bf16)
    slot = tag * CAP
    for m in range(MEMBERS):
        mark = jnp.where(tag == m, 1.0, 0.0)
        slot = slot + mark * jnp.dot(earlier, mark.astype(bf16), preferred_element_type=f32)
    lane = lax.broadcasted_iota(i32, spread_ref.shape, 1)
    pair = spread_ref.shape[1] // (MEMBERS * CAP)
    wanted = lane // (pair * CAP) * CAP + lane % CAP
    spread_ref[...] = jnp.where(slot == wanted.astype(f32), 1.0, 0.0).astype(bf16)
    place = jnp.where(slot == lane.astype(f32), 1.0, 0.0).astype(bf16)
    place_ref[...] = place[:, : place_ref.shape[1]]


def share_kernel(xs, x_ref, rows_ref, gate_ref, up_ref, *refs):
    others, (out_ref, weights, out, weight_sem, out_sem) = refs[: xs - 1], refs[xs - 1 :]
    x = x_ref[0]
    depth = weights.shape[1]
    mine = pl.ds(pl.multiple_of(x * depth, depth), depth)
    parts = xs
    per = out_ref.shape[0] // parts
    loads = [[pltpu.make_async_copy(ref, weights.at[k + 1], weight_sem.at[k])] for k, ref in enumerate(others)]
    loads.append(
        [
            pltpu.make_async_copy(
                ref.at[0, mine], weights.at[0, :, i * LANES : (i + 1) * LANES], weight_sem.at[xs - 1 + i]
            )
            for i, ref in enumerate((gate_ref, up_ref))
        ]
    )
    for load in loads:
        for copy in load:
            copy.start()
    sends = []
    for q in range(parts):
        at = slice(q * per, (q + 1) * per)
        for load, k in zip(loads, (*range(1, xs), 0)):
            if q == 0:
                for copy in load:
                    copy.wait()
            source = lax.rem(x - k + xs, xs)
            gate_at = pl.multiple_of(source * LANES, LANES)
            up_at = pl.multiple_of((source + xs) * LANES, LANES)
            part = jnp.dot(rows_ref[at, :], weights[k], preferred_element_type=f32).astype(bf16)
            out[at, pl.ds(gate_at, LANES)] = part[:, :LANES]
            out[at, pl.ds(up_at, LANES)] = part[:, LANES:]
        send = pltpu.make_async_copy(out.at[at], out_ref.at[at], out_sem.at[q])
        send.start()
        sends.append(send)
    for send in sends:
        send.wait()


def down_kernel(xs, x_ref, share_ref, w0_ref, w1_ref, w3_ref, w2a_ref, w2b_ref, out_ref, hid_ref):
    x = x_ref[0]
    both = share_ref[0].astype(f32)
    for q in range(1, xs):
        both = both + share_ref[q].astype(f32)
    units = xs * LANES
    hid_ref[...] = (jax.nn.silu(both[:, :units]) * both[:, units:]).astype(bf16)
    mine = [
        hid_ref[:, pl.ds(pl.multiple_of(lax.rem(x - k + xs, xs) * LANES, LANES), LANES)]
        for k in range(xs)
    ]
    half = LANES // 2
    step = 512
    for n in range(0, out_ref.shape[1], step):
        cols = slice(n, n + step)
        total = jnp.dot(mine[0], w0_ref[:, cols], preferred_element_type=f32)
        total += jnp.dot(mine[1], w1_ref[:, cols], preferred_element_type=f32)
        total += jnp.dot(mine[3], w3_ref[:, cols], preferred_element_type=f32)
        total += jnp.dot(mine[2][:, :half], w2a_ref[:, cols], preferred_element_type=f32)
        total += jnp.dot(mine[2][:, half:], w2b_ref[:, cols], preferred_element_type=f32)
        out_ref[:, cols] = total.astype(bf16)


def held(arrays):
    return [pltpu.with_memory_space_constraint(a, pltpu.HBM) for a in arrays]


def small(kernel, shapes, *args, in_specs=None):
    many = isinstance(shapes, (tuple, list))
    return pl.pallas_call(
        kernel,
        out_shape=shapes,
        in_specs=in_specs or [VMEM] * len(args),
        out_specs=[VMEM] * len(shapes) if many else VMEM,
        compiler_params=pltpu.CompilerParams(vmem_limit_bytes=1 << 20),
    )(*args)


def body(tokens, expert_ids, combine_codes, gate_weight, up_weight, down_weight):
    nodes = lax.axis_size("z") * lax.axis_size("core")
    ys, xs = lax.axis_size("y"), lax.axis_size("x")
    pair = ys // MEMBERS
    token_count, width = tokens.shape
    chunk = width // xs
    units = gate_weight.shape[2]
    x = lax.axis_index("x")
    x_arg = x.astype(i32)[None]

    target = expert_ids // MEMBERS
    member = expert_ids % MEMBERS
    named = target[None, :, :] == jnp.arange(nodes, dtype=i32)[:, None, None]
    pick = jnp.any(named, axis=2).astype(bf16)
    slot_member = jnp.sum(jnp.where(named, member[None], 0), axis=(1, 2))
    outgoing = jnp.dot(pick, tokens, preferred_element_type=f32).astype(bf16)
    tag = jnp.broadcast_to(slot_member.astype(bf16)[:, None, None], (nodes, xs, LANES))
    outgoing = jnp.concatenate([outgoing.reshape(nodes, xs, chunk), tag], axis=2)
    arrived = exchange(outgoing, NODE)
    weights = small(weight_kernel, jax.ShapeDtypeStruct((TOP, token_count), f32), combine_codes.T)

    joined = jnp.concatenate([gate_weight[0], up_weight[0]], axis=1)
    blocks = []
    for k in range(1, xs):
        block = lax.dynamic_slice_in_dim(joined, lax.rem(x + k, xs) * chunk, chunk, 0)
        blocks.append(shift(block, k, xs))
    down = down_weight[0]
    down_left = shift(down, 1, xs)
    down_right = shift(down, xs - 1, xs)
    half = units // 2
    down_far_a = shift(down_left[:half], 1, xs)
    down_far_b = shift(down_right[half:], xs - 1, xs)

    place, spread = pl.pallas_call(
        slot_kernel,
        grid=(1,),
        out_shape=(
            jax.ShapeDtypeStruct((nodes, MEMBERS * CAP), bf16),
            jax.ShapeDtypeStruct((nodes, ys * CAP), bf16),
        ),
        in_specs=[pl.BlockSpec((nodes, xs, LANES), lambda i: (0, 0, chunk // LANES))],
        out_specs=(
            pl.BlockSpec((nodes, MEMBERS * CAP), lambda i: (0, 0)),
            pl.BlockSpec((nodes, ys * CAP), lambda i: (0, 0)),
        ),
        compiler_params=pltpu.CompilerParams(vmem_limit_bytes=1 << 20),
    )(arrived)
    bundle = jnp.dot(place.T, arrived.reshape(nodes, -1), preferred_element_type=f32).astype(bf16)
    bundle = bundle.reshape(MEMBERS, 1, CAP, xs, chunk + LANES)[..., :chunk].transpose(3, 0, 1, 2, 4)
    bundle = jnp.broadcast_to(bundle, (xs, MEMBERS, pair, CAP, chunk)).reshape(xs * ys, CAP, chunk)
    cores = lax.axis_size("core")
    by_core = spread.reshape(nodes // cores, cores, -1).transpose(1, 0, 2).reshape(spread.shape)
    target = small(target_kernel, jax.ShapeDtypeStruct((TOP, token_count), i32), expert_ids.T)
    rows = exchange(bundle, LOCAL).reshape(xs * ys * CAP, chunk)

    share_shape = (xs * ys * CAP, 2 * xs * units)
    share = pl.pallas_call(
        functools.partial(share_kernel, xs),
        out_shape=pltpu.HBM(share_shape, bf16),
        in_specs=[SMEM, VMEM] + [HBM] * (1 + xs),
        out_specs=HBM,
        scratch_shapes=[
            pltpu.VMEM((xs, chunk, 2 * units), bf16),
            pltpu.VMEM(share_shape, bf16),
            pltpu.SemaphoreType.DMA((xs + 1,)),
            pltpu.SemaphoreType.DMA((xs,)),
        ],
        compiler_params=pltpu.CompilerParams(vmem_limit_bytes=20 << 20),
        cost_estimate=pl.CostEstimate(flops=2 << 30, bytes_accessed=4 << 20, transcendentals=0),
    )(x_arg, rows, *held((gate_weight, up_weight, *blocks)))
    share = exchange(share.reshape(xs, ys * CAP, 2 * xs * units), "x")
    partial_out = pl.pallas_call(
        functools.partial(down_kernel, xs),
        out_shape=jax.ShapeDtypeStruct((ys * CAP, width), bf16),
        in_specs=[SMEM] + [VMEM] * 6,
        out_specs=VMEM,
        scratch_shapes=[pltpu.VMEM((ys * CAP, xs * units), bf16)],
        compiler_params=pltpu.CompilerParams(vmem_limit_bytes=16 << 20),
        cost_estimate=pl.CostEstimate(flops=1 << 30, bytes_accessed=6 << 20, transcendentals=1 << 16),
    )(x_arg, share, down, down_left, down_right, down_far_a, down_far_b)
    returned = exchange(partial_out.reshape(ys, CAP, width), "y").reshape(ys * CAP, width)

    results = jnp.dot(by_core, returned, preferred_element_type=f32).astype(bf16)
    results = exchange(results.reshape(cores, nodes // cores, xs, chunk), "core")
    results = results.transpose(1, 0, 2, 3)
    terms = small(mix_kernel, jax.ShapeDtypeStruct((nodes, 2 * token_count), bf16), target, weights)
    home = exchange(results, "z").reshape(nodes, width)
    mixed = jnp.dot(terms.T, home, preferred_element_type=f32)
    return (mixed[:token_count] + mixed[token_count:]).astype(bf16)


def solution(mesh):
    nodes, locals_ = mesh.shape["node"], mesh.shape["local"]
    split = Mesh(mesh.devices.reshape(nodes // 2, 2, locals_ // 4, 4), ALL)
    in_specs = (
        P(ALL, None),
        P(ALL, None),
        P(ALL, None),
        P(ALL, None, None),
        P(ALL, None, None),
        P(ALL, None, None),
    )

    return jax.shard_map(body, mesh=split, in_specs=in_specs, out_specs=P(ALL, None), check_vma=False)
```

```python
import functools

import jax
import jax.numpy as jnp
from jax import lax
from jax.experimental import pallas as pl
from jax.experimental.pallas import tpu as pltpu
from jax.sharding import Mesh
from jax.sharding import PartitionSpec as P

TOP = 4
MEMBERS = 4
CAP = 16
LANES = 128
NODE = ("z", "core")
LOCAL = ("x", "y")
ALL = ("z", "core", "y", "x")
f32, bf16, i32 = jnp.float32, jnp.bfloat16, jnp.int32
VMEM = pl.BlockSpec(memory_space=pltpu.VMEM)
SMEM = pl.BlockSpec(memory_space=pltpu.SMEM)
HBM = pl.BlockSpec(memory_space=pltpu.HBM)


def exchange(value, axes):
    return lax.all_to_all(value, axes, split_axis=0, concat_axis=0, tiled=True)


def shift(value, by, count):
    return lax.ppermute(value, "x", [(i, (i + by) % count) for i in range(count)])


def weight_kernel(codes_ref, out_ref):
    codes = codes_ref[...].astype(f32)
    out_ref[...] = codes / jnp.sum(codes, axis=0, keepdims=True)


def target_kernel(ids_ref, out_ref):
    out_ref[...] = ids_ref[...] // MEMBERS


def mix_kernel(target_ref, weights_ref, out_ref):
    tokens = target_ref.shape[1]
    node = lax.broadcasted_iota(i32, (out_ref.shape[0], tokens), 0)
    mix = jnp.zeros(node.shape, f32)
    for k in range(TOP):
        mix = mix + jnp.where(target_ref[k : k + 1, :] == node, weights_ref[k : k + 1, :], 0.0)
    high = mix.astype(bf16)
    out_ref[:, :tokens] = high
    out_ref[:, tokens:] = (mix - high.astype(f32)).astype(bf16)


def place_kernel(pair, rows_ref, out_ref, spread_ref, bundle, sem):
    xs, nodes, _ = rows_ref.shape
    chunk = bundle.shape[-1]
    tag = rows_ref[0, :, chunk:].astype(f32)
    row = lax.broadcasted_iota(i32, (nodes, nodes), 0)
    column = lax.broadcasted_iota(i32, (nodes, nodes), 1)
    earlier = jnp.where(column < row, 1.0, 0.0).astype(bf16)
    slot = tag * CAP
    for m in range(MEMBERS):
        mark = jnp.where(tag == m, 1.0, 0.0)
        slot = slot + mark * jnp.dot(earlier, mark.astype(bf16), preferred_element_type=f32)
    lane = lax.broadcasted_iota(i32, slot.shape, 1)
    place = jnp.where(slot == lane.astype(f32), 1.0, 0.0).astype(bf16)[:, : MEMBERS * CAP]
    sends = []
    for q in range(xs):
        held_rows = lax.dot_general(
            place, rows_ref[q, :, :chunk], (((0,), (0,)), ((), ())), preferred_element_type=f32
        )
        bundle[q] = held_rows.astype(bf16).reshape(MEMBERS, CAP, chunk)
        for p in range(pair):
            send = pltpu.make_async_copy(bundle.at[q], out_ref.at[q, :, p], sem.at[q * pair + p])
            send.start()
            sends.append(send)
    wanted = lane // (pair * CAP) * CAP + lane % CAP
    spread_ref[...] = jnp.where(slot == wanted.astype(f32), 1.0, 0.0).astype(bf16)
    for send in sends:
        send.wait()


def share_kernel(xs, x_ref, rows_ref, gate_ref, up_ref, *refs):
    others, (out_ref, weights, out, weight_sem, out_sem) = refs[: xs - 1], refs[xs - 1 :]
    x = x_ref[0]
    depth = weights.shape[1]
    mine = pl.ds(pl.multiple_of(x * depth, depth), depth)
    parts = xs
    per = out_ref.shape[0] // parts
    loads = [[pltpu.make_async_copy(ref, weights.at[k + 1], weight_sem.at[k])] for k, ref in enumerate(others)]
    loads.append(
        [
            pltpu.make_async_copy(
                ref.at[0, mine], weights.at[0, :, i * LANES : (i + 1) * LANES], weight_sem.at[xs - 1 + i]
            )
            for i, ref in enumerate((gate_ref, up_ref))
        ]
    )
    for load in loads:
        for copy in load:
            copy.start()
    sends = []
    for q in range(parts):
        at = slice(q * per, (q + 1) * per)
        for load, k in zip(loads, (*range(1, xs), 0)):
            if q == 0:
                for copy in load:
                    copy.wait()
            source = lax.rem(x - k + xs, xs)
            gate_at = pl.multiple_of(source * LANES, LANES)
            up_at = pl.multiple_of((source + xs) * LANES, LANES)
            part = jnp.dot(rows_ref[at, :], weights[k], preferred_element_type=f32).astype(bf16)
            out[at, pl.ds(gate_at, LANES)] = part[:, :LANES]
            out[at, pl.ds(up_at, LANES)] = part[:, LANES:]
        send = pltpu.make_async_copy(out.at[at], out_ref.at[at], out_sem.at[q])
        send.start()
        sends.append(send)
    for send in sends:
        send.wait()


def down_kernel(xs, x_ref, share_ref, w0_ref, w1_ref, w3_ref, w2a_ref, w2b_ref, out_ref, hid_ref):
    x = x_ref[0]
    both = share_ref[0].astype(f32)
    for q in range(1, xs):
        both = both + share_ref[q].astype(f32)
    units = xs * LANES
    hid_ref[...] = (jax.nn.silu(both[:, :units]) * both[:, units:]).astype(bf16)
    mine = [
        hid_ref[:, pl.ds(pl.multiple_of(lax.rem(x - k + xs, xs) * LANES, LANES), LANES)]
        for k in range(xs)
    ]
    half = LANES // 2
    step = 512
    for n in range(0, out_ref.shape[1], step):
        cols = slice(n, n + step)
        total = jnp.dot(mine[0], w0_ref[:, cols], preferred_element_type=f32)
        total += jnp.dot(mine[1], w1_ref[:, cols], preferred_element_type=f32)
        total += jnp.dot(mine[3], w3_ref[:, cols], preferred_element_type=f32)
        total += jnp.dot(mine[2][:, :half], w2a_ref[:, cols], preferred_element_type=f32)
        total += jnp.dot(mine[2][:, half:], w2b_ref[:, cols], preferred_element_type=f32)
        out_ref[:, cols] = total.astype(bf16)


def held(arrays):
    return [pltpu.with_memory_space_constraint(a, pltpu.HBM) for a in arrays]


def small(kernel, shapes, *args, in_specs=None):
    many = isinstance(shapes, (tuple, list))
    return pl.pallas_call(
        kernel,
        out_shape=shapes,
        in_specs=in_specs or [VMEM] * len(args),
        out_specs=[VMEM] * len(shapes) if many else VMEM,
        compiler_params=pltpu.CompilerParams(vmem_limit_bytes=1 << 20),
    )(*args)


def body(tokens, expert_ids, combine_codes, gate_weight, up_weight, down_weight):
    nodes = lax.axis_size("z") * lax.axis_size("core")
    ys, xs = lax.axis_size("y"), lax.axis_size("x")
    pair = ys // MEMBERS
    token_count, width = tokens.shape
    chunk = width // xs
    units = gate_weight.shape[2]
    x = lax.axis_index("x")
    x_arg = x.astype(i32)[None]

    target = expert_ids // MEMBERS
    member = expert_ids % MEMBERS
    cores = lax.axis_size("core")
    named = target[None, :, :] == jnp.arange(nodes, dtype=i32)[:, None, None]
    pick = jnp.any(named, axis=2).astype(bf16)
    slot_member = jnp.sum(jnp.where(named, member[None], 0), axis=(1, 2))
    outgoing = jnp.dot(pick, tokens, preferred_element_type=f32).astype(bf16)
    tag = jnp.broadcast_to(slot_member.astype(bf16)[:, None, None], (nodes, xs, LANES))
    outgoing = jnp.concatenate([outgoing.reshape(nodes, xs, chunk), tag], axis=2)
    arrived = exchange(outgoing, NODE)
    weights = small(weight_kernel, jax.ShapeDtypeStruct((TOP, token_count), f32), combine_codes.T)

    joined = jnp.concatenate([gate_weight[0], up_weight[0]], axis=1)
    blocks = []
    for k in range(1, xs):
        block = lax.dynamic_slice_in_dim(joined, lax.rem(x + k, xs) * chunk, chunk, 0)
        blocks.append(shift(block, k, xs))
    down = down_weight[0]
    down_left = shift(down, 1, xs)
    down_right = shift(down, xs - 1, xs)
    half = units // 2
    down_far_a = shift(down_left[:half], 1, xs)
    down_far_b = shift(down_right[half:], xs - 1, xs)

    bundle, spread = pl.pallas_call(
        functools.partial(place_kernel, pair),
        out_shape=(
            pltpu.HBM((xs, MEMBERS, pair, CAP, chunk), bf16),
            jax.ShapeDtypeStruct((nodes, ys * CAP), bf16),
        ),
        in_specs=[VMEM],
        out_specs=(HBM, VMEM),
        scratch_shapes=[
            pltpu.VMEM((xs, MEMBERS, CAP, chunk), bf16),
            pltpu.SemaphoreType.DMA((xs * pair,)),
        ],
        compiler_params=pltpu.CompilerParams(vmem_limit_bytes=8 << 20),
    )(arrived.transpose(1, 0, 2))
    bundle = bundle.reshape(xs * ys, CAP, chunk)
    by_core = spread.reshape(nodes // cores, cores, -1).transpose(1, 0, 2).reshape(spread.shape)
    target = small(target_kernel, jax.ShapeDtypeStruct((TOP, token_count), i32), expert_ids.T)
    rows = exchange(bundle, LOCAL).reshape(xs * ys * CAP, chunk)

    share_shape = (xs * ys * CAP, 2 * xs * units)
    share = pl.pallas_call(
        functools.partial(share_kernel, xs),
        out_shape=pltpu.HBM(share_shape, bf16),
        in_specs=[SMEM, VMEM] + [HBM] * (1 + xs),
        out_specs=HBM,
        scratch_shapes=[
            pltpu.VMEM((xs, chunk, 2 * units), bf16),
            pltpu.VMEM(share_shape, bf16),
            pltpu.SemaphoreType.DMA((xs + 1,)),
            pltpu.SemaphoreType.DMA((xs,)),
        ],
        compiler_params=pltpu.CompilerParams(vmem_limit_bytes=20 << 20),
        cost_estimate=pl.CostEstimate(flops=2 << 30, bytes_accessed=4 << 20, transcendentals=0),
    )(x_arg, rows, *held((gate_weight, up_weight, *blocks)))
    share = exchange(share.reshape(xs, ys * CAP, 2 * xs * units), "x")
    partial_out = pl.pallas_call(
        functools.partial(down_kernel, xs),
        out_shape=jax.ShapeDtypeStruct((ys * CAP, width), bf16),
        in_specs=[SMEM] + [VMEM] * 6,
        out_specs=VMEM,
        scratch_shapes=[pltpu.VMEM((ys * CAP, xs * units), bf16)],
        compiler_params=pltpu.CompilerParams(vmem_limit_bytes=16 << 20),
        cost_estimate=pl.CostEstimate(flops=1 << 30, bytes_accessed=6 << 20, transcendentals=1 << 16),
    )(x_arg, share, *held((down,)), down_left, down_right, down_far_a, down_far_b)
    returned = exchange(partial_out.reshape(ys, CAP, width), "y").reshape(ys * CAP, width)

    results = jnp.dot(by_core, returned, preferred_element_type=f32).astype(bf16)
    results = exchange(results.reshape(cores, nodes // cores, xs, chunk), "core")
    results = results.transpose(1, 0, 2, 3)
    terms = small(mix_kernel, jax.ShapeDtypeStruct((nodes, 2 * token_count), bf16), target, weights)
    home = exchange(results, "z").reshape(nodes, width)
    mixed = jnp.dot(terms.T, home, preferred_element_type=f32)
    return (mixed[:token_count] + mixed[token_count:]).astype(bf16)


def solution(mesh):
    nodes, locals_ = mesh.shape["node"], mesh.shape["local"]
    split = Mesh(mesh.devices.reshape(nodes // 2, 2, locals_ // 4, 4), ALL)
    in_specs = (
        P(ALL, None),
        P(ALL, None),
        P(ALL, None),
        P(ALL, None, None),
        P(ALL, None, None),
        P(ALL, None, None),
    )

    return jax.shard_map(body, mesh=split, in_specs=in_specs, out_specs=P(ALL, None), check_vma=False)
```

```python
import functools

import jax
import jax.numpy as jnp
from jax import lax
from jax.experimental import pallas as pl
from jax.experimental.pallas import tpu as pltpu
from jax.sharding import Mesh
from jax.sharding import PartitionSpec as P

TOP = 4
MEMBERS = 4
CAP = 16
LANES = 128
NODE = ("z", "core")
LOCAL = ("x", "y")
ALL = ("z", "core", "y", "x")
f32, bf16, i32 = jnp.float32, jnp.bfloat16, jnp.int32
VMEM = pl.BlockSpec(memory_space=pltpu.VMEM)
SMEM = pl.BlockSpec(memory_space=pltpu.SMEM)
HBM = pl.BlockSpec(memory_space=pltpu.HBM)


def exchange(value, axes):
    return lax.all_to_all(value, axes, split_axis=0, concat_axis=0, tiled=True)


def shift(value, by, count):
    return lax.ppermute(value, "x", [(i, (i + by) % count) for i in range(count)])


def weight_kernel(codes_ref, out_ref):
    codes = codes_ref[...].astype(f32)
    out_ref[...] = codes / jnp.sum(codes, axis=0, keepdims=True)


def target_kernel(ids_ref, out_ref):
    out_ref[...] = ids_ref[...] // MEMBERS


def mix_kernel(target_ref, weights_ref, out_ref):
    tokens = target_ref.shape[1]
    node = lax.broadcasted_iota(i32, (out_ref.shape[0], tokens), 0)
    mix = jnp.zeros(node.shape, f32)
    for k in range(TOP):
        mix = mix + jnp.where(target_ref[k : k + 1, :] == node, weights_ref[k : k + 1, :], 0.0)
    high = mix.astype(bf16)
    out_ref[:, :tokens] = high
    out_ref[:, tokens:] = (mix - high.astype(f32)).astype(bf16)


def place_kernel(pair, cores, rows_ref, out_ref, spread_ref, bundle, sem):
    xs, nodes, _ = rows_ref.shape
    chunk = bundle.shape[-1]
    tag = rows_ref[0, :, chunk:].astype(f32)
    row = lax.broadcasted_iota(i32, (nodes, nodes), 0)
    column = lax.broadcasted_iota(i32, (nodes, nodes), 1)
    earlier = jnp.where(column < row, 1.0, 0.0).astype(bf16)
    slot = tag * CAP
    for m in range(MEMBERS):
        mark = jnp.where(tag == m, 1.0, 0.0)
        slot = slot + mark * jnp.dot(earlier, mark.astype(bf16), preferred_element_type=f32)
    lane = lax.broadcasted_iota(i32, slot.shape, 1)
    place = jnp.where(slot == lane.astype(f32), 1.0, 0.0).astype(bf16)[:, : MEMBERS * CAP]
    sends = []
    for q in range(xs):
        held_rows = lax.dot_general(
            place, rows_ref[q, :, :chunk], (((0,), (0,)), ((), ())), preferred_element_type=f32
        )
        bundle[q] = held_rows.astype(bf16).reshape(MEMBERS, CAP, chunk)
        for p in range(pair):
            send = pltpu.make_async_copy(bundle.at[q], out_ref.at[q, :, p], sem.at[q * pair + p])
            send.start()
            sends.append(send)
    wanted = lane // (pair * CAP) * CAP + lane % CAP
    spread = jnp.where(slot == wanted.astype(f32), 1.0, 0.0).astype(bf16)
    by_core = row % (nodes // cores) * cores + row // (nodes // cores)
    turn = jnp.where(column == by_core, 1.0, 0.0).astype(bf16)
    spread_ref[...] = jnp.dot(turn, spread, preferred_element_type=f32).astype(bf16)
    for send in sends:
        send.wait()


def share_kernel(xs, x_ref, rows_ref, gate_ref, up_ref, *refs):
    others, (out_ref, weights, out, weight_sem, out_sem) = refs[: xs - 1], refs[xs - 1 :]
    x = x_ref[0]
    depth = weights.shape[1]
    mine = pl.ds(pl.multiple_of(x * depth, depth), depth)
    parts = xs
    per = out_ref.shape[0] // parts
    loads = [[pltpu.make_async_copy(ref, weights.at[k + 1], weight_sem.at[k])] for k, ref in enumerate(others)]
    loads.append(
        [
            pltpu.make_async_copy(
                ref.at[0, mine], weights.at[0, :, i * LANES : (i + 1) * LANES], weight_sem.at[xs - 1 + i]
            )
            for i, ref in enumerate((gate_ref, up_ref))
        ]
    )
    for load in loads:
        for copy in load:
            copy.start()
    sends = []
    for q in range(parts):
        at = slice(q * per, (q + 1) * per)
        for load, k in zip(loads, (*range(1, xs), 0)):
            if q == 0:
                for copy in load:
                    copy.wait()
            source = lax.rem(x - k + xs, xs)
            gate_at = pl.multiple_of(source * LANES, LANES)
            up_at = pl.multiple_of((source + xs) * LANES, LANES)
            part = jnp.dot(rows_ref[at, :], weights[k], preferred_element_type=f32).astype(bf16)
            out[at, pl.ds(gate_at, LANES)] = part[:, :LANES]
            out[at, pl.ds(up_at, LANES)] = part[:, LANES:]
        send = pltpu.make_async_copy(out.at[at], out_ref.at[at], out_sem.at[q])
        send.start()
        sends.append(send)
    for send in sends:
        send.wait()


def down_kernel(xs, x_ref, share_ref, w0_ref, w1_ref, w3_ref, w2a_ref, w2b_ref, out_ref, hid_ref):
    x = x_ref[0]
    both = share_ref[0].astype(f32)
    for q in range(1, xs):
        both = both + share_ref[q].astype(f32)
    units = xs * LANES
    hid_ref[...] = (jax.nn.silu(both[:, :units]) * both[:, units:]).astype(bf16)
    mine = [
        hid_ref[:, pl.ds(pl.multiple_of(lax.rem(x - k + xs, xs) * LANES, LANES), LANES)]
        for k in range(xs)
    ]
    half = LANES // 2
    step = 512
    for n in range(0, out_ref.shape[1], step):
        cols = slice(n, n + step)
        total = jnp.dot(mine[0], w0_ref[:, cols], preferred_element_type=f32)
        total += jnp.dot(mine[1], w1_ref[:, cols], preferred_element_type=f32)
        total += jnp.dot(mine[3], w3_ref[:, cols], preferred_element_type=f32)
        total += jnp.dot(mine[2][:, :half], w2a_ref[:, cols], preferred_element_type=f32)
        total += jnp.dot(mine[2][:, half:], w2b_ref[:, cols], preferred_element_type=f32)
        out_ref[:, cols] = total.astype(bf16)


def held(arrays):
    return [pltpu.with_memory_space_constraint(a, pltpu.HBM) for a in arrays]


def small(kernel, shapes, *args, in_specs=None):
    many = isinstance(shapes, (tuple, list))
    return pl.pallas_call(
        kernel,
        out_shape=shapes,
        in_specs=in_specs or [VMEM] * len(args),
        out_specs=[VMEM] * len(shapes) if many else VMEM,
        compiler_params=pltpu.CompilerParams(vmem_limit_bytes=1 << 20),
    )(*args)


def body(tokens, expert_ids, combine_codes, gate_weight, up_weight, down_weight):
    nodes = lax.axis_size("z") * lax.axis_size("core")
    ys, xs = lax.axis_size("y"), lax.axis_size("x")
    pair = ys // MEMBERS
    token_count, width = tokens.shape
    chunk = width // xs
    units = gate_weight.shape[2]
    x = lax.axis_index("x")
    x_arg = x.astype(i32)[None]

    target = expert_ids // MEMBERS
    member = expert_ids % MEMBERS
    cores = lax.axis_size("core")
    named = target[None, :, :] == jnp.arange(nodes, dtype=i32)[:, None, None]
    pick = jnp.any(named, axis=2).astype(bf16)
    slot_member = jnp.sum(jnp.where(named, member[None], 0), axis=(1, 2))
    outgoing = jnp.dot(pick, tokens, preferred_element_type=f32).astype(bf16)
    tag = jnp.broadcast_to(slot_member.astype(bf16)[:, None, None], (nodes, xs, LANES))
    outgoing = jnp.concatenate([outgoing.reshape(nodes, xs, chunk), tag], axis=2)
    arrived = exchange(outgoing, NODE)
    weights = small(weight_kernel, jax.ShapeDtypeStruct((TOP, token_count), f32), combine_codes.T)

    joined = jnp.concatenate([gate_weight[0], up_weight[0]], axis=1)
    blocks = []
    for k in range(1, xs):
        block = lax.dynamic_slice_in_dim(joined, lax.rem(x + k, xs) * chunk, chunk, 0)
        blocks.append(shift(block, k, xs))
    down = down_weight[0]
    down_left = shift(down, 1, xs)
    down_right = shift(down, xs - 1, xs)
    half = units // 2
    down_far_a = shift(down_left[:half], 1, xs)
    down_far_b = shift(down_right[half:], xs - 1, xs)

    bundle, spread = pl.pallas_call(
        functools.partial(place_kernel, pair, cores),
        out_shape=(
            pltpu.HBM((xs, MEMBERS, pair, CAP, chunk), bf16),
            jax.ShapeDtypeStruct((nodes, ys * CAP), bf16),
        ),
        in_specs=[VMEM],
        out_specs=(HBM, VMEM),
        scratch_shapes=[
            pltpu.VMEM((xs, MEMBERS, CAP, chunk), bf16),
            pltpu.SemaphoreType.DMA((xs * pair,)),
        ],
        compiler_params=pltpu.CompilerParams(vmem_limit_bytes=8 << 20),
    )(arrived.transpose(1, 0, 2))
    bundle = bundle.reshape(xs * ys, CAP, chunk)
    target = small(target_kernel, jax.ShapeDtypeStruct((TOP, token_count), i32), expert_ids.T)
    rows = exchange(bundle, LOCAL).reshape(xs * ys * CAP, chunk)

    share_shape = (xs * ys * CAP, 2 * xs * units)
    share = pl.pallas_call(
        functools.partial(share_kernel, xs),
        out_shape=pltpu.HBM(share_shape, bf16),
        in_specs=[SMEM, VMEM] + [HBM] * (1 + xs),
        out_specs=HBM,
        scratch_shapes=[
            pltpu.VMEM((xs, chunk, 2 * units), bf16),
            pltpu.VMEM(share_shape, bf16),
            pltpu.SemaphoreType.DMA((xs + 1,)),
            pltpu.SemaphoreType.DMA((xs,)),
        ],
        compiler_params=pltpu.CompilerParams(vmem_limit_bytes=20 << 20),
        cost_estimate=pl.CostEstimate(flops=2 << 30, bytes_accessed=4 << 20, transcendentals=0),
    )(x_arg, rows, *held((gate_weight, up_weight, *blocks)))
    share = exchange(share.reshape(xs, ys * CAP, 2 * xs * units), "x")
    partial_out = pl.pallas_call(
        functools.partial(down_kernel, xs),
        out_shape=jax.ShapeDtypeStruct((ys * CAP, width), bf16),
        in_specs=[SMEM] + [VMEM] * 6,
        out_specs=VMEM,
        scratch_shapes=[pltpu.VMEM((ys * CAP, xs * units), bf16)],
        compiler_params=pltpu.CompilerParams(vmem_limit_bytes=16 << 20),
        cost_estimate=pl.CostEstimate(flops=1 << 30, bytes_accessed=6 << 20, transcendentals=1 << 16),
    )(x_arg, share, *held((down,)), down_left, down_right, down_far_a, down_far_b)
    returned = exchange(partial_out.reshape(ys, CAP, width), "y").reshape(ys * CAP, width)

    results = jnp.dot(spread, returned, preferred_element_type=f32).astype(bf16)
    results = exchange(results.reshape(cores, nodes // cores, xs, chunk), "core")
    results = results.transpose(1, 0, 2, 3)
    terms = small(mix_kernel, jax.ShapeDtypeStruct((nodes, 2 * token_count), bf16), target, weights)
    home = exchange(results, "z").reshape(nodes, width)
    mixed = jnp.dot(terms.T, home, preferred_element_type=f32)
    return (mixed[:token_count] + mixed[token_count:]).astype(bf16)


def solution(mesh):
    nodes, locals_ = mesh.shape["node"], mesh.shape["local"]
    split = Mesh(mesh.devices.reshape(nodes // 2, 2, locals_ // 4, 4), ALL)
    in_specs = (
        P(ALL, None),
        P(ALL, None),
        P(ALL, None),
        P(ALL, None, None),
        P(ALL, None, None),
        P(ALL, None, None),
    )

    return jax.shard_map(body, mesh=split, in_specs=in_specs, out_specs=P(ALL, None), check_vma=False)
```

```python
import functools

import jax
import jax.numpy as jnp
from jax import lax
from jax.experimental import pallas as pl
from jax.experimental.pallas import tpu as pltpu
from jax.sharding import Mesh
from jax.sharding import PartitionSpec as P

TOP = 4
MEMBERS = 4
CAP = 16
LANES = 128
NODE = ("z", "core")
LOCAL = ("x", "y")
ALL = ("z", "core", "y", "x")
f32, bf16, i32 = jnp.float32, jnp.bfloat16, jnp.int32
VMEM = pl.BlockSpec(memory_space=pltpu.VMEM)
SMEM = pl.BlockSpec(memory_space=pltpu.SMEM)
HBM = pl.BlockSpec(memory_space=pltpu.HBM)


def exchange(value, axes):
    return lax.all_to_all(value, axes, split_axis=0, concat_axis=0, tiled=True)


def shift(value, by, count):
    return lax.ppermute(value, "x", [(i, (i + by) % count) for i in range(count)])


def weight_kernel(codes_ref, out_ref):
    codes = codes_ref[...].astype(f32)
    out_ref[...] = codes / jnp.sum(codes, axis=0, keepdims=True)


def target_kernel(ids_ref, out_ref):
    out_ref[...] = ids_ref[...] // MEMBERS


def mix_kernel(target_ref, weights_ref, out_ref):
    tokens = target_ref.shape[1]
    node = lax.broadcasted_iota(i32, (out_ref.shape[0], tokens), 0)
    mix = jnp.zeros(node.shape, f32)
    for k in range(TOP):
        mix = mix + jnp.where(target_ref[k : k + 1, :] == node, weights_ref[k : k + 1, :], 0.0)
    high = mix.astype(bf16)
    out_ref[:, :tokens] = high
    out_ref[:, tokens:] = (mix - high.astype(f32)).astype(bf16)


def place_kernel(pair, cores, rows_ref, out_ref, spread_ref, bundle, sem):
    xs, nodes, _ = rows_ref.shape
    chunk = bundle.shape[-1]
    tag = rows_ref[0, :, chunk:].astype(f32)
    row = lax.broadcasted_iota(i32, (nodes, nodes), 0)
    column = lax.broadcasted_iota(i32, (nodes, nodes), 1)
    earlier = jnp.where(column < row, 1.0, 0.0).astype(bf16)
    slot = tag * CAP
    for m in range(MEMBERS):
        mark = jnp.where(tag == m, 1.0, 0.0)
        slot = slot + mark * jnp.dot(earlier, mark.astype(bf16), preferred_element_type=f32)
    lane = lax.broadcasted_iota(i32, slot.shape, 1)
    place = jnp.where(slot == lane.astype(f32), 1.0, 0.0).astype(bf16)[:, : MEMBERS * CAP]
    sends = []
    for q in range(xs):
        held_rows = lax.dot_general(
            place, rows_ref[q, :, :chunk], (((0,), (0,)), ((), ())), preferred_element_type=f32
        )
        bundle[q] = held_rows.astype(bf16).reshape(MEMBERS, CAP, chunk)
        for p in range(pair):
            send = pltpu.make_async_copy(bundle.at[q], out_ref.at[q, :, p], sem.at[q * pair + p])
            send.start()
            sends.append(send)
    wanted = lane // (pair * CAP) * CAP + lane % CAP
    spread = jnp.where(slot == wanted.astype(f32), 1.0, 0.0).astype(bf16)
    by_core = row % (nodes // cores) * cores + row // (nodes // cores)
    turn = jnp.where(column == by_core, 1.0, 0.0).astype(bf16)
    spread_ref[...] = jnp.dot(turn, spread, preferred_element_type=f32).astype(bf16)
    for send in sends:
        send.wait()


def block_kernel(xs, x_ref, gate_ref, up_ref, *refs):
    outs, (buffer, load_sem, send_sem) = refs[: xs - 1], refs[xs - 1 :]
    x = x_ref[0]
    depth = buffer.shape[1]
    loads = []
    for k in range(1, xs):
        rows = pl.ds(pl.multiple_of(lax.rem(x + k, xs) * depth, depth), depth)
        loads.append(
            [
                pltpu.make_async_copy(
                    ref.at[0, rows], buffer.at[k - 1, :, i * LANES : (i + 1) * LANES], load_sem.at[k - 1, i]
                )
                for i, ref in enumerate((gate_ref, up_ref))
            ]
        )
    for load in loads:
        for copy in load:
            copy.start()
    sends = []
    for k, load in enumerate(loads):
        for copy in load:
            copy.wait()
        send = pltpu.make_async_copy(buffer.at[k], outs[k], send_sem.at[k])
        send.start()
        sends.append(send)
    for send in sends:
        send.wait()


def share_kernel(xs, x_ref, rows_ref, gate_ref, up_ref, *refs):
    others, (out_ref, weights, out, weight_sem, out_sem) = refs[: xs - 1], refs[xs - 1 :]
    x = x_ref[0]
    depth = weights.shape[1]
    mine = pl.ds(pl.multiple_of(x * depth, depth), depth)
    parts = xs
    per = out_ref.shape[0] // parts
    loads = [[pltpu.make_async_copy(ref, weights.at[k + 1], weight_sem.at[k])] for k, ref in enumerate(others)]
    loads.append(
        [
            pltpu.make_async_copy(
                ref.at[0, mine], weights.at[0, :, i * LANES : (i + 1) * LANES], weight_sem.at[xs - 1 + i]
            )
            for i, ref in enumerate((gate_ref, up_ref))
        ]
    )
    for load in loads:
        for copy in load:
            copy.start()
    sends = []
    for q in range(parts):
        at = slice(q * per, (q + 1) * per)
        for load, k in zip(loads, (*range(1, xs), 0)):
            if q == 0:
                for copy in load:
                    copy.wait()
            source = lax.rem(x - k + xs, xs)
            gate_at = pl.multiple_of(source * LANES, LANES)
            up_at = pl.multiple_of((source + xs) * LANES, LANES)
            part = jnp.dot(rows_ref[at, :], weights[k], preferred_element_type=f32).astype(bf16)
            out[at, pl.ds(gate_at, LANES)] = part[:, :LANES]
            out[at, pl.ds(up_at, LANES)] = part[:, LANES:]
        send = pltpu.make_async_copy(out.at[at], out_ref.at[at], out_sem.at[q])
        send.start()
        sends.append(send)
    for send in sends:
        send.wait()


def down_kernel(xs, x_ref, share_ref, w0_ref, w1_ref, w3_ref, w2a_ref, w2b_ref, out_ref, hid_ref):
    x = x_ref[0]
    both = share_ref[0].astype(f32)
    for q in range(1, xs):
        both = both + share_ref[q].astype(f32)
    units = xs * LANES
    hid_ref[...] = (jax.nn.silu(both[:, :units]) * both[:, units:]).astype(bf16)
    mine = [
        hid_ref[:, pl.ds(pl.multiple_of(lax.rem(x - k + xs, xs) * LANES, LANES), LANES)]
        for k in range(xs)
    ]
    half = LANES // 2
    step = 512
    for n in range(0, out_ref.shape[1], step):
        cols = slice(n, n + step)
        total = jnp.dot(mine[0], w0_ref[:, cols], preferred_element_type=f32)
        total += jnp.dot(mine[1], w1_ref[:, cols], preferred_element_type=f32)
        total += jnp.dot(mine[3], w3_ref[:, cols], preferred_element_type=f32)
        total += jnp.dot(mine[2][:, :half], w2a_ref[:, cols], preferred_element_type=f32)
        total += jnp.dot(mine[2][:, half:], w2b_ref[:, cols], preferred_element_type=f32)
        out_ref[:, cols] = total.astype(bf16)


def held(arrays):
    return [pltpu.with_memory_space_constraint(a, pltpu.HBM) for a in arrays]


def small(kernel, shapes, *args, in_specs=None):
    many = isinstance(shapes, (tuple, list))
    return pl.pallas_call(
        kernel,
        out_shape=shapes,
        in_specs=in_specs or [VMEM] * len(args),
        out_specs=[VMEM] * len(shapes) if many else VMEM,
        compiler_params=pltpu.CompilerParams(vmem_limit_bytes=1 << 20),
    )(*args)


def body(tokens, expert_ids, combine_codes, gate_weight, up_weight, down_weight):
    nodes = lax.axis_size("z") * lax.axis_size("core")
    ys, xs = lax.axis_size("y"), lax.axis_size("x")
    pair = ys // MEMBERS
    token_count, width = tokens.shape
    chunk = width // xs
    units = gate_weight.shape[2]
    x = lax.axis_index("x")
    x_arg = x.astype(i32)[None]

    target = expert_ids // MEMBERS
    member = expert_ids % MEMBERS
    cores = lax.axis_size("core")
    named = target[None, :, :] == jnp.arange(nodes, dtype=i32)[:, None, None]
    pick = jnp.any(named, axis=2).astype(bf16)
    slot_member = jnp.sum(jnp.where(named, member[None], 0), axis=(1, 2))
    outgoing = jnp.dot(pick, tokens, preferred_element_type=f32).astype(bf16)
    tag = jnp.broadcast_to(slot_member.astype(bf16)[:, None, None], (nodes, xs, LANES))
    outgoing = jnp.concatenate([outgoing.reshape(nodes, xs, chunk), tag], axis=2)
    arrived = exchange(outgoing, NODE)
    weights = small(weight_kernel, jax.ShapeDtypeStruct((TOP, token_count), f32), combine_codes.T)

    quarters = pl.pallas_call(
        functools.partial(block_kernel, xs),
        out_shape=[pltpu.HBM((chunk, 2 * units), bf16)] * (xs - 1),
        in_specs=[SMEM, HBM, HBM],
        out_specs=[HBM] * (xs - 1),
        scratch_shapes=[
            pltpu.VMEM((xs - 1, chunk, 2 * units), bf16),
            pltpu.SemaphoreType.DMA((xs - 1, 2)),
            pltpu.SemaphoreType.DMA((xs - 1,)),
        ],
        compiler_params=pltpu.CompilerParams(vmem_limit_bytes=8 << 20),
        cost_estimate=pl.CostEstimate(flops=1 << 20, bytes_accessed=3 << 20, transcendentals=0),
    )(x_arg, *held((gate_weight, up_weight)))
    blocks = []
    for k in range(1, xs):
        blocks.append(shift(quarters[k - 1], k, xs))
    down = down_weight[0]
    down_left = shift(down, 1, xs)
    down_right = shift(down, xs - 1, xs)
    half = units // 2
    down_far_a = shift(down_left[:half], 1, xs)
    down_far_b = shift(down_right[half:], xs - 1, xs)

    bundle, spread = pl.pallas_call(
        functools.partial(place_kernel, pair, cores),
        out_shape=(
            pltpu.HBM((xs, MEMBERS, pair, CAP, chunk), bf16),
            jax.ShapeDtypeStruct((nodes, ys * CAP), bf16),
        ),
        in_specs=[VMEM],
        out_specs=(HBM, VMEM),
        scratch_shapes=[
            pltpu.VMEM((xs, MEMBERS, CAP, chunk), bf16),
            pltpu.SemaphoreType.DMA((xs * pair,)),
        ],
        compiler_params=pltpu.CompilerParams(vmem_limit_bytes=8 << 20),
    )(arrived.transpose(1, 0, 2))
    bundle = bundle.reshape(xs * ys, CAP, chunk)
    target = small(target_kernel, jax.ShapeDtypeStruct((TOP, token_count), i32), expert_ids.T)
    rows = exchange(bundle, LOCAL).reshape(xs * ys * CAP, chunk)

    share_shape = (xs * ys * CAP, 2 * xs * units)
    share = pl.pallas_call(
        functools.partial(share_kernel, xs),
        out_shape=pltpu.HBM(share_shape, bf16),
        in_specs=[SMEM, VMEM] + [HBM] * (1 + xs),
        out_specs=HBM,
        scratch_shapes=[
            pltpu.VMEM((xs, chunk, 2 * units), bf16),
            pltpu.VMEM(share_shape, bf16),
            pltpu.SemaphoreType.DMA((xs + 1,)),
            pltpu.SemaphoreType.DMA((xs,)),
        ],
        compiler_params=pltpu.CompilerParams(vmem_limit_bytes=20 << 20),
        cost_estimate=pl.CostEstimate(flops=2 << 30, bytes_accessed=4 << 20, transcendentals=0),
    )(x_arg, rows, *held((gate_weight, up_weight, *blocks)))
    share = exchange(share.reshape(xs, ys * CAP, 2 * xs * units), "x")
    partial_out = pl.pallas_call(
        functools.partial(down_kernel, xs),
        out_shape=jax.ShapeDtypeStruct((ys * CAP, width), bf16),
        in_specs=[SMEM] + [VMEM] * 6,
        out_specs=VMEM,
        scratch_shapes=[pltpu.VMEM((ys * CAP, xs * units), bf16)],
        compiler_params=pltpu.CompilerParams(vmem_limit_bytes=16 << 20),
        cost_estimate=pl.CostEstimate(flops=1 << 30, bytes_accessed=6 << 20, transcendentals=1 << 16),
    )(x_arg, share, *held((down,)), down_left, down_right, down_far_a, down_far_b)
    returned = exchange(partial_out.reshape(ys, CAP, width), "y").reshape(ys * CAP, width)

    results = jnp.dot(spread, returned, preferred_element_type=f32).astype(bf16)
    results = exchange(results.reshape(cores, nodes // cores, xs, chunk), "core")
    results = results.transpose(1, 0, 2, 3)
    terms = small(mix_kernel, jax.ShapeDtypeStruct((nodes, 2 * token_count), bf16), target, weights)
    home = exchange(results, "z").reshape(nodes, width)
    mixed = jnp.dot(terms.T, home, preferred_element_type=f32)
    return (mixed[:token_count] + mixed[token_count:]).astype(bf16)


def solution(mesh):
    nodes, locals_ = mesh.shape["node"], mesh.shape["local"]
    split = Mesh(mesh.devices.reshape(nodes // 2, 2, locals_ // 4, 4), ALL)
    in_specs = (
        P(ALL, None),
        P(ALL, None),
        P(ALL, None),
        P(ALL, None, None),
        P(ALL, None, None),
        P(ALL, None, None),
    )

    return jax.shard_map(body, mesh=split, in_specs=in_specs, out_specs=P(ALL, None), check_vma=False)
```
